32 devices in a mesh: prompt: 4 (over y, x), resp: 8 (over z, core).
Axes of the slice: x: 2, y: 2, z: 4, core: 2. Of those that a mesh axis runs over, the one named last changes fastest.
Arguments:
- embeddings: bfloat16 [32, 256, 3584], P('prompt', 'resp'), parts along dimension 0, may hold values from -6 to 6
- head_weight: bfloat16 [3584, 3584], P('resp'), may hold values from -0.0017089844 to 0.0017089844
- valid_mask: int32 [32, 256], P('prompt', 'resp'), parts along dimension 0, may hold values from 0 to 1, as said below
Outputs:
- preferences: float32 [32, 256, 256], P('prompt', 'resp'), parts along dimension 0
- win_rates: float32 [32, 256], P('prompt', 'resp'), parts along dimension 0
The draws below stay inside these ranges and needn't reach their ends.
There are 4 independent parts, one for each index of `prompt`. The reference program is written for one: setup_inputs(seed, part) draws one part's arguments, and reference() takes and returns one part's arrays. A program takes and returns all parts, laid end to end along the dimension named above; an argument that names none is the same for every part. Nothing has to cross between parts.
Inputs may be any that keep to these rules, and one draw needn't show every extreme that they name: `valid_mask`: for each prompt the ones are its first response slots, between 64 and 256 of them; in every draw some prompt has all 256 slots filled.
All inputs are finite; a program needn't handle non-finite values.
Results may differ from the reference program's by a relative error of at most 0.003.
Values may be sent and summed in bfloat16 or wider, within the bound.
A program may use at most 128 MiB of HBM per device.

```python
import jax
import jax.numpy as jnp
from jax import lax

D = 3584
PROMPTS = 8
RESP = 256


def draw_valid_mask(key, part):
    first, second, third = jax.random.split(key, 3)
    lengths = jax.random.randint(first, (PROMPTS,), RESP // 4, RESP + 1)
    prompt_ids = jnp.arange(PROMPTS, dtype=jnp.int32)
    shortest = jax.random.randint(second, (), 0, PROMPTS)
    longest = jax.random.randint(third, (), 0, PROMPTS)
    lengths = jnp.where(prompt_ids == shortest, RESP // 4, lengths)
    lengths = jnp.where(prompt_ids == longest, RESP, lengths)
    slot_ids = jnp.arange(RESP, dtype=jnp.int32)
    return (slot_ids[None, :] < lengths[:, None]).astype(jnp.int32)


def block_levels(rng, shape, cuts, smallest, largest):
    loudness = 1.0
    for position, shards_of in cuts:
        steps = jax.random.uniform(jax.random.fold_in(jax.random.fold_in(rng, 6), position), (shards_of,), jnp.float32, smallest / len(cuts), largest / len(cuts))
        loudness = loudness * jnp.repeat(jnp.exp(steps), shape[position] // shards_of).reshape((-1,) + (1,) * (len(shape) - 1 - position))
    return loudness


def noise(stream_key, dims, deviation, most, pieces=(), held_as=jnp.bfloat16):
    drawn = deviation * jax.random.normal(stream_key, dims, jnp.float32)
    if pieces:
        drawn = drawn * block_levels(stream_key, dims, pieces, -0.22, 0.18)
    return jnp.clip(drawn, -most, most).astype(held_as)


def setup_inputs(seed: int = 0, part: int = 0) -> dict:
    keys = jax.random.split(jax.random.key(seed), 4)
    part_keys = jax.random.split(jax.random.fold_in(keys[3], part), 4)
    return {
        "embeddings": noise(part_keys[0], (PROMPTS, RESP, D), 1.0, 6.0, ((1, 8),)),
        "head_weight": noise(keys[1], (D, D), (D * D) ** -0.5, 0.0017089844, ((0, 8),)),
        "valid_mask": draw_valid_mask(jax.random.fold_in(jax.random.fold_in(keys[3], part), 71), part),
    }


def reference(embeddings, head_weight, valid_mask):
    flat_rows = embeddings.reshape(PROMPTS * RESP, D)
    direct = jnp.dot(flat_rows, head_weight, preferred_element_type=jnp.float32)
    mirror = lax.dot_general(flat_rows, head_weight, (((1,), (1,)), ((), ())), preferred_element_type=jnp.float32)
    projected = (direct - mirror).astype(jnp.bfloat16).reshape(PROMPTS, RESP, D)

    def one_prompt(pair):
        rows_in, proj_in = pair
        return -jnp.dot(rows_in, proj_in.T, preferred_element_type=jnp.float32)

    scores = lax.map(one_prompt, (embeddings, projected))
    valid = valid_mask.astype(jnp.float32)
    counts = jnp.sum(valid, axis=1)
    preferences = jax.nn.sigmoid(scores) * valid[:, :, None] * valid[:, None, :]
    totals = jnp.sum(preferences, axis=2) - 0.5 * valid
    win_rates = valid * totals / jnp.maximum(counts - 1.0, 1.0)[:, None]
    return preferences, win_rates
```

```python
import jax
import jax.numpy as jnp
from jax import lax
from jax.sharding import PartitionSpec as P


def halves_of_scores(embeddings, head_weight, own_index, group_size):
    prompts, block_rows, features = embeddings.shape
    held = head_weight.shape[0]
    slots = group_size * block_rows
    everyone = lax.all_gather(embeddings, "resp", axis=0, tiled=True)
    flat = everyone.reshape(group_size * prompts * block_rows, features)
    through = lax.dot_general(
        flat, head_weight, (((1,), (1,)), ((), ())), preferred_element_type=jnp.float32
    ).astype(jnp.bfloat16)
    through = through.reshape(group_size, prompts, block_rows, held)
    mine = lax.dynamic_slice_in_dim(
        everyone.reshape(group_size, prompts, block_rows, features), own_index * held, held, 3
    )
    partial = jnp.einsum("gpid,hpjd->gpihj", mine, through, preferred_element_type=jnp.float32)
    flipped = jnp.einsum("gpid,hpjd->gpihj", through, mine, preferred_element_type=jnp.float32)
    partial = (partial - flipped).astype(jnp.bfloat16)
    return partial.reshape(group_size, prompts, block_rows, slots)


def shards(embeddings, head_weight, valid_mask):
    group_size = lax.axis_size("resp")
    own_index = lax.axis_index("resp")
    prompts, block_rows, features = embeddings.shape
    slots = group_size * block_rows
    valid_rows = valid_mask.astype(jnp.float32)
    counts = lax.psum(jnp.sum(valid_rows, axis=1), "resp")
    at_once = max(1, min(prompts, (1 << 11) // slots))

    def scores_of(some):
        partial = halves_of_scores(some, head_weight, own_index, group_size)
        swapped = lax.all_to_all(partial, "resp", split_axis=0, concat_axis=0, tiled=True)
        return jnp.sum(swapped.astype(jnp.float32), axis=0)

    if at_once == prompts:
        scores = scores_of(embeddings)
    else:
        scores = lax.map(scores_of, embeddings.reshape(prompts // at_once, at_once, block_rows, features))
        scores = scores.reshape(prompts, block_rows, slots)
    column_ids = jnp.arange(slots, dtype=jnp.float32)
    valid_cols = (column_ids[None, :] < counts[:, None]).astype(jnp.float32)
    preferences = jax.nn.sigmoid(scores) * valid_rows[:, :, None] * valid_cols[:, None, :]
    totals = jnp.sum(preferences, axis=2) - 0.5 * valid_rows
    win_rates = valid_rows * totals / jnp.maximum(counts - 1.0, 1.0)[:, None]
    return (preferences, win_rates)


def solution(mesh):
    return jax.shard_map(
        shards,
        mesh=mesh,
        in_specs=(P("prompt", "resp", None), P("resp", None), P("prompt", "resp")),
        out_specs=(P("prompt", "resp", None), P("prompt", "resp")),
        check_vma=False,
    )
```

```python
import functools

import jax
import jax.numpy as jnp
from jax import lax
from jax.experimental import pallas as pl
from jax.experimental.pallas import tpu as pltpu
from jax.sharding import PartitionSpec as P

MESH = pl.DeviceIdType.MESH
CORES = 2
CHIPS = 4
PARTS = 4
NT = (((1,), (1,)), ((), ()))


def gathered_halves(embeddings, head_weight, own_index, group_size):
    prompts, block_rows, features = embeddings.shape
    held = head_weight.shape[0]
    slots = group_size * block_rows
    everyone = lax.all_gather(embeddings, "resp", axis=0, tiled=True)
    flat = everyone.reshape(group_size * prompts * block_rows, features)
    through = lax.dot_general(flat, head_weight, NT, preferred_element_type=jnp.float32)
    through = through.astype(jnp.bfloat16).reshape(group_size, prompts, block_rows, held)
    mine = lax.dynamic_slice_in_dim(
        everyone.reshape(group_size, prompts, block_rows, features), own_index * held, held, 3
    )
    partial = jnp.einsum("gpid,hpjd->gpihj", mine, through, preferred_element_type=jnp.float32)
    flipped = jnp.einsum("gpid,hpjd->gpihj", through, mine, preferred_element_type=jnp.float32)
    partial = (partial - flipped).astype(jnp.bfloat16)
    return partial.reshape(group_size, prompts, block_rows, slots)


def gathered_scores(embeddings, head_weight):
    group_size = lax.axis_size("resp")
    own_index = lax.axis_index("resp")
    prompts, block_rows, features = embeddings.shape
    slots = group_size * block_rows
    at_once = max(1, min(prompts, (1 << 11) // slots))

    def scores_of(some):
        partial = gathered_halves(some, head_weight, own_index, group_size)
        swapped = lax.all_to_all(partial, "resp", split_axis=0, concat_axis=0, tiled=True)
        return jnp.sum(swapped.astype(jnp.float32), axis=0)

    pieces = embeddings.reshape(prompts // at_once, at_once, block_rows, features)
    return lax.map(scores_of, pieces).reshape(prompts, block_rows, slots)


def kernel(e_ref, w_ref, m_ref, s_ref, g_ref,
           ebuf, wbuf, zbuf, sbuf, keep, pbuf, qbuf, fbuf, rbuf, mbuf,
           m_send, m_recv, e_send, e_recv, ef_send, el_sem,
           w_send, w_recv, wl_sem, p_send, p_recv, f_send, r_recv):
    part = lax.axis_index("prompt")
    me = lax.axis_index("resp")
    z = me // CORES
    core = me % CORES
    half = z // 2
    prompts, block_rows, features = e_ref.shape
    held = w_ref.shape[0]
    per_core = prompts // CORES
    group = CHIPS * CORES
    span = held * group // 2
    rows = group * block_rows
    half_rows = rows // 2
    z_in = 1 + half
    z_out = 3 * half
    z_far = 2 - half
    far_out = 3 - z_out
    inner = z == z_in
    quarter = held // PARTS
    width = 256 if span % 256 == 0 else span

    def copy(src, dst, send, recv, chip, c, q=None):
        return pltpu.make_async_remote_copy(
            src, dst, send, recv,
            device_id=(part if q is None else q, chip * CORES + c), device_id_type=MESH,
        )

    def arrived(dst, recv):
        copy(dst, dst, m_send.at[0], recv, z_far, core).wait_recv()

    others = [lax.rem(me + d, group) for d in range(1, group)]
    plane = [lax.rem(part + d, PARTS) for d in range(1, PARTS)]
    barrier = pltpu.get_barrier_semaphore()
    for other in others:
        pl.semaphore_signal(barrier, inc=1, device_id=(part, other), device_id_type=MESH)
    for q in plane:
        pl.semaphore_signal(barrier, inc=1, device_id=(q, me), device_id_type=MESH)
    pl.semaphore_wait(barrier, len(others) + len(plane))

    def w_rows(block, start, size):
        return wbuf.at[pl.ds(pl.multiple_of(block * held + start, 16), size)]

    def mask_copy(d):
        return pltpu.make_async_remote_copy(
            m_ref, mbuf.at[me], m_send.at[d], m_recv.at[me],
            device_id=(part, others[d]), device_id_type=MESH,
        )

    my_block = me - half * group // 2
    out_block = z_out * CORES + core - half * group // 2
    out_other = z_out * CORES + 1 - core - half * group // 2
    in_other = z_in * CORES + 1 - core - half * group // 2
    my_quarter = pl.multiple_of(part * quarter, 16)

    def outer_w():
        return copy(w_ref.at[pl.ds(my_quarter, quarter)], w_rows(my_block, my_quarter, quarter),
                    w_send.at[0], w_recv.at[part], z_in, core)

    def outer_e(j, c):
        return copy(e_ref.at[c * per_core + j], ebuf.at[j, me],
                    e_send.at[j, c], e_recv.at[j, me], z_in, c)

    def far_e(j, c):
        return copy(e_ref.at[c * per_core + j], ebuf.at[j, me],
                    e_send.at[j, c], e_recv.at[j, me], z_far, c)

    def near_e(j):
        return copy(e_ref.at[(1 - core) * per_core + j], ebuf.at[j, me],
                    e_send.at[j, 2], e_recv.at[j, me], z_in, 1 - core)

    def own_e(j):
        return pltpu.make_async_copy(e_ref.at[core * per_core + j], ebuf.at[j, me], el_sem.at[j])

    def onward_e(j, c):
        spot = ebuf.at[j, z_out * CORES + c]
        return copy(spot, spot, ef_send.at[j, c], e_recv.at[j, z_out * CORES + c], z_far, core)

    def near_w():
        return copy(w_ref, w_rows(my_block, 0, held), w_send.at[0], w_recv.at[PARTS], z_in, 1 - core)

    def own_w():
        return pltpu.make_async_copy(w_ref, w_rows(my_block, 0, held), wl_sem.at[0])

    def plane_w(d):
        spot = w_rows(out_block, my_quarter, quarter)
        return copy(spot, spot, w_send.at[1 + d], w_recv.at[part], z_in, core, plane[d])

    def across_w():
        spot = w_rows(out_block, 0, held)
        return copy(spot, spot, w_send.at[PARTS], w_recv.at[PARTS + 1], z_in, 1 - core)

    def partial_copy(j):
        return copy(pbuf.at[j], qbuf.at[j], p_send.at[j], p_recv.at[j], z_far, core)

    def final_copy(j, t):
        target = half * (group // 2) + lax.rem(my_block + 1 + t, group // 2)
        row = pl.multiple_of(lax.rem(my_block + 1 + t, group // 2) * block_rows, block_rows)
        return pltpu.make_async_remote_copy(
            fbuf.at[j, pl.ds(row, block_rows)], rbuf.at[core * per_core + j],
            f_send.at[j, t], r_recv.at[core * per_core + j],
            device_id=(part, target), device_id_type=MESH,
        )

    @pl.when(jnp.logical_not(inner))
    def _():
        outer_w().start()
        for j in range(per_core):
            for c in range(CORES):
                outer_e(j, c).start()

    @pl.when(inner)
    def _():
        for j in range(per_core):
            for c in range(CORES):
                far_e(j, c).start()
        near_w().start()
        for j in range(per_core):
            near_e(j).start()
        own_w().start()
        for j in range(per_core):
            own_e(j).start()

    for d in range(group - 1):
        mask_copy(d).start()
    mbuf[me] = m_ref[...]

    @pl.when(inner)
    def _():
        arrived(w_rows(out_block, my_quarter, quarter), w_recv.at[part])
        for d in range(PARTS - 1):
            plane_w(d).start()

        def pass_on(j, carry):
            for c in range(CORES):
                arrived(ebuf.at[j, z_out * CORES + c], e_recv.at[j, z_out * CORES + c])
                onward_e(j, c).start()
            return carry

        lax.fori_loop(0, per_core, pass_on, 0)
        for q in plane:
            arrived(w_rows(out_block, q * quarter, quarter), w_recv.at[q])
        across_w().start()
        own_w().wait()
        arrived(w_rows(in_other, 0, held), w_recv.at[PARTS])
        arrived(w_rows(out_other, 0, held), w_recv.at[PARTS + 1])

        mine_at = pl.multiple_of(half * half_rows, half_rows)
        theirs_at = pl.multiple_of((1 - half) * half_rows, half_rows)
        lanes = pl.ds(pl.multiple_of(half * span, 128), span)

        def finish(j):
            arrived(qbuf.at[j], p_recv.at[j])
            fbuf[j] = (keep[j] + qbuf[j].astype(jnp.float32)).astype(jnp.bfloat16)
            for t in range(group // 2 - 1):
                final_copy(j, t).start()
            own_row = pl.multiple_of(my_block * block_rows, block_rows)
            rbuf[core * per_core + j] = fbuf[j, pl.ds(own_row, block_rows)]

        def score(j, carry):
            own_e(j).wait()
            arrived(ebuf.at[j, z_in * CORES + 1 - core], e_recv.at[j, z_in * CORES + 1 - core])
            for chip in (z_far, far_out):
                for c in range(CORES):
                    arrived(ebuf.at[j, chip * CORES + c], e_recv.at[j, chip * CORES + c])

            def project(k, inside):
                start = pl.multiple_of(k * width, width)
                left = ebuf[j].reshape(rows, features)
                zbuf[:, pl.ds(start, width)] = lax.dot_general(
                    left, wbuf[pl.ds(start, width)], NT, preferred_element_type=jnp.float32
                ).astype(jnp.bfloat16)
                return inside

            lax.fori_loop(0, span // width, project, 0)
            left = ebuf[j, :, :, lanes].reshape(rows, span)
            right = zbuf[...]
            sbuf[...] = lax.dot_general(
                left, right, NT, preferred_element_type=jnp.float32
            ) - lax.dot_general(right, left, NT, preferred_element_type=jnp.float32)
            pbuf[j] = sbuf[pl.ds(theirs_at, half_rows)].astype(jnp.bfloat16)
            partial_copy(j).start()
            keep[j] = sbuf[pl.ds(mine_at, half_rows)]

            @pl.when(j > 0)
            def _():
                finish(j - 1)

            return carry

        lax.fori_loop(0, per_core, score, 0)
        finish(per_core - 1)
        for j in range(per_core):
            arrived(rbuf.at[(1 - core) * per_core + j], r_recv.at[(1 - core) * per_core + j])
        for j in range(per_core):
            for c in range(CORES):
                far_e(j, c).wait_send()
                onward_e(j, c).wait_send()
            near_e(j).wait_send()
            partial_copy(j).wait_send()
            for t in range(group // 2 - 1):
                final_copy(j, t).wait_send()
        near_w().wait_send()
        across_w().wait_send()
        for d in range(PARTS - 1):
            plane_w(d).wait_send()

    @pl.when(jnp.logical_not(inner))
    def _():
        outer_w().wait_send()
        for j in range(per_core):
            for c in range(CORES):
                outer_e(j, c).wait_send()
        for p in range(prompts):
            arrived(rbuf.at[p], r_recv.at[p])

    for d in range(group - 1):
        mask_copy(d).wait_send()
        arrived(mbuf.at[others[d]], m_recv.at[others[d]])
    s_ref[...] = rbuf[...]
    g_ref[...] = mbuf[...]


def line_scores(embeddings, head_weight, mask):
    prompts, block_rows, features = embeddings.shape
    held = head_weight.shape[0]
    group = CHIPS * CORES
    per_core = prompts // CORES
    span = held * group // 2
    rows = group * block_rows
    half_rows = rows // 2
    bf16, f32 = jnp.bfloat16, jnp.float32
    dma = pltpu.SemaphoreType.DMA
    anywhere = pl.BlockSpec(memory_space=pl.ANY)
    vmem = pl.BlockSpec(memory_space=pltpu.VMEM)
    padded = jnp.pad(mask, ((0, 0), (0, 128 - block_rows)))
    return pl.pallas_call(
        kernel,
        out_shape=(
            jax.ShapeDtypeStruct((prompts, block_rows, rows), bf16),
            jax.ShapeDtypeStruct((group, prompts, 128), jnp.int32),
        ),
        in_specs=[anywhere, anywhere, vmem],
        out_specs=(vmem, vmem),
        scratch_shapes=[
            pltpu.VMEM((per_core, group, block_rows, features), bf16),
            pltpu.VMEM((span, features), bf16),
            pltpu.VMEM((rows, span), bf16),
            pltpu.VMEM((rows, rows), f32),
            pltpu.VMEM((per_core, half_rows, rows), f32),
            pltpu.VMEM((per_core, half_rows, rows), bf16),
            pltpu.VMEM((per_core, half_rows, rows), bf16),
            pltpu.VMEM((per_core, half_rows, rows), bf16),
            pltpu.VMEM((prompts, block_rows, rows), bf16),
            pltpu.VMEM((group, prompts, 128), jnp.int32),
            dma((group - 1,)),
            dma((group,)),
            dma((per_core, 3)),
            dma((per_core, group)),
            dma((per_core, CORES)),
            dma((per_core,)),
            dma((PARTS + 1,)),
            dma((PARTS + 2,)),
            dma((1,)),
            dma((per_core,)),
            dma((per_core,)),
            dma((per_core, group // 2 - 1)),
            dma((prompts,)),
        ],
        compiler_params=pltpu.CompilerParams(
            collective_id=0, has_side_effects=True, vmem_limit_bytes=56 << 20
        ),
    )(embeddings, head_weight, padded)


def shards(embeddings, head_weight, valid_mask):
    group_size = lax.axis_size("resp")
    prompts, block_rows, features = embeddings.shape
    slots = group_size * block_rows
    valid_rows = valid_mask.astype(jnp.float32)
    if (lax.axis_size("prompt"), group_size) == (PARTS, CHIPS * CORES):
        scores, masks = line_scores(embeddings, head_weight, valid_mask)
        scores = scores.astype(jnp.float32)
        valid_cols = jnp.transpose(masks[:, :, :block_rows], (1, 0, 2)).reshape(prompts, slots)
        valid_cols = valid_cols.astype(jnp.float32)
        counts = jnp.sum(valid_cols, axis=1)
    else:
        counts = lax.psum(jnp.sum(valid_rows, axis=1), "resp")
        scores = gathered_scores(embeddings, head_weight)
        column_ids = jnp.arange(slots, dtype=jnp.float32)
        valid_cols = (column_ids[None, :] < counts[:, None]).astype(jnp.float32)
    preferences = jax.nn.sigmoid(scores) * valid_rows[:, :, None] * valid_cols[:, None, :]
    totals = jnp.sum(preferences, axis=2) - 0.5 * valid_rows
    win_rates = valid_rows * totals / jnp.maximum(counts - 1.0, 1.0)[:, None]
    return (preferences, win_rates)


def solution(mesh):
    return jax.shard_map(
        shards,
        mesh=mesh,
        in_specs=(P("prompt", "resp", None), P("resp", None), P("prompt", "resp")),
        out_specs=(P("prompt", "resp", None), P("prompt", "resp")),
        check_vma=False,
    )
```

```python
import functools

import jax
import jax.numpy as jnp
from jax import lax
from jax.experimental import pallas as pl
from jax.experimental.pallas import tpu as pltpu
from jax.sharding import PartitionSpec as P

MESH = pl.DeviceIdType.MESH
CORES = 2
CHIPS = 4
PARTS = 4
NT = (((1,), (1,)), ((), ()))


def gathered_halves(embeddings, head_weight, own_index, group_size):
    prompts, block_rows, features = embeddings.shape
    held = head_weight.shape[0]
    slots = group_size * block_rows
    everyone = lax.all_gather(embeddings, "resp", axis=0, tiled=True)
    flat = everyone.reshape(group_size * prompts * block_rows, features)
    through = lax.dot_general(flat, head_weight, NT, preferred_element_type=jnp.float32)
    through = through.astype(jnp.bfloat16).reshape(group_size, prompts, block_rows, held)
    mine = lax.dynamic_slice_in_dim(
        everyone.reshape(group_size, prompts, block_rows, features), own_index * held, held, 3
    )
    partial = jnp.einsum("gpid,hpjd->gpihj", mine, through, preferred_element_type=jnp.float32)
    flipped = jnp.einsum("gpid,hpjd->gpihj", through, mine, preferred_element_type=jnp.float32)
    partial = (partial - flipped).astype(jnp.bfloat16)
    return partial.reshape(group_size, prompts, block_rows, slots)


def gathered_scores(embeddings, head_weight):
    group_size = lax.axis_size("resp")
    own_index = lax.axis_index("resp")
    prompts, block_rows, features = embeddings.shape
    slots = group_size * block_rows
    at_once = max(1, min(prompts, (1 << 11) // slots))

    def scores_of(some):
        partial = gathered_halves(some, head_weight, own_index, group_size)
        swapped = lax.all_to_all(partial, "resp", split_axis=0, concat_axis=0, tiled=True)
        return jnp.sum(swapped.astype(jnp.float32), axis=0)

    pieces = embeddings.reshape(prompts // at_once, at_once, block_rows, features)
    return lax.map(scores_of, pieces).reshape(prompts, block_rows, slots)


def kernel(e_ref, w_ref, m_ref, o_ref, r_ref,
           ebuf, wbuf, zbuf, sbuf, keep, pbuf, qbuf, fbuf, rbuf, mine_cols, mbuf,
           m_send, m_recv, e_send, e_recv, ef_send, el_sem,
           w_send, w_recv, wl_sem, p_send, p_recv, f_send, r_recv):
    part = lax.axis_index("prompt")
    me = lax.axis_index("resp")
    z = me // CORES
    core = me % CORES
    half = z // 2
    prompts, block_rows, features = e_ref.shape
    held = w_ref.shape[0]
    per_core = prompts // CORES
    group = CHIPS * CORES
    span = held * group // 2
    rows = group * block_rows
    half_rows = rows // 2
    z_in = 1 + half
    z_out = 3 * half
    z_far = 2 - half
    far_out = 3 - z_out
    inner = z == z_in
    quarter = held // PARTS
    width = 256 if span % 256 == 0 else span

    def copy(src, dst, send, recv, chip, c, q=None):
        return pltpu.make_async_remote_copy(
            src, dst, send, recv,
            device_id=(part if q is None else q, chip * CORES + c), device_id_type=MESH,
        )

    def arrived(dst, recv):
        copy(dst, dst, m_send.at[0], recv, z_far, core).wait_recv()

    valid = m_ref[...].astype(jnp.float32)
    slot = lax.broadcasted_iota(jnp.int32, (block_rows, rows), 1) - me * block_rows
    place = (slot == lax.broadcasted_iota(jnp.int32, (block_rows, rows), 0)).astype(jnp.float32)
    mine_cols[...] = jnp.dot(valid, place, preferred_element_type=jnp.float32).astype(jnp.int32)

    others = [lax.rem(me + d, group) for d in range(1, group)]
    plane = [lax.rem(part + d, PARTS) for d in range(1, PARTS)]
    barrier = pltpu.get_barrier_semaphore()
    for other in others:
        pl.semaphore_signal(barrier, inc=1, device_id=(part, other), device_id_type=MESH)
    for q in plane:
        pl.semaphore_signal(barrier, inc=1, device_id=(q, me), device_id_type=MESH)
    pl.semaphore_wait(barrier, len(others) + len(plane))

    def w_rows(block, start, size):
        return wbuf.at[pl.ds(pl.multiple_of(block * held + start, 16), size)]

    def mask_copy(d):
        return pltpu.make_async_remote_copy(
            mine_cols, mbuf.at[me], m_send.at[d], m_recv.at[me],
            device_id=(part, others[d]), device_id_type=MESH,
        )

    my_block = me - half * group // 2
    out_block = z_out * CORES + core - half * group // 2
    out_other = z_out * CORES + 1 - core - half * group // 2
    in_other = z_in * CORES + 1 - core - half * group // 2
    my_quarter = pl.multiple_of(part * quarter, 16)
    first = quarter // 32 * 16
    pieces = ((0, first), (first, quarter - first))

    def outer_w(i):
        at, size = pieces[i]
        return copy(w_ref.at[pl.ds(pl.multiple_of(my_quarter + at, 16), size)],
                    w_rows(my_block, my_quarter + at, size),
                    w_send.at[0, i], w_recv.at[part, i], z_in, core)

    def outer_e(j, c):
        return copy(e_ref.at[c * per_core + j], ebuf.at[j, me],
                    e_send.at[j, c], e_recv.at[j, me], z_in, c)

    def far_e(j, c):
        return copy(e_ref.at[c * per_core + j], ebuf.at[j, me],
                    e_send.at[j, c], e_recv.at[j, me], z_far, c)

    def near_e(j):
        return copy(e_ref.at[(1 - core) * per_core + j], ebuf.at[j, me],
                    e_send.at[j, 2], e_recv.at[j, me], z_in, 1 - core)

    def own_e(j):
        return pltpu.make_async_copy(e_ref.at[core * per_core + j], ebuf.at[j, me], el_sem.at[j])

    def onward_e(j, c):
        spot = ebuf.at[j, z_out * CORES + c]
        return copy(spot, spot, ef_send.at[j, c], e_recv.at[j, z_out * CORES + c], z_far, core)

    def near_w():
        return copy(w_ref, w_rows(my_block, 0, held), w_send.at[0, 0], w_recv.at[PARTS, 0], z_in, 1 - core)

    def own_w():
        return pltpu.make_async_copy(w_ref, w_rows(my_block, 0, held), wl_sem.at[0])

    def plane_w(d, i):
        at, size = pieces[i]
        spot = w_rows(out_block, my_quarter + at, size)
        return copy(spot, spot, w_send.at[1 + d, i], w_recv.at[part, i], z_in, core, plane[d])

    def across_w():
        spot = w_rows(out_block, 0, held)
        return copy(spot, spot, w_send.at[PARTS, 0], w_recv.at[PARTS, 1], z_in, 1 - core)

    def partial_copy(j):
        return copy(pbuf.at[j], qbuf.at[j], p_send.at[j], p_recv.at[j], z_far, core)

    def final_copy(j, t):
        target = half * (group // 2) + lax.rem(my_block + 1 + t, group // 2)
        row = pl.multiple_of(lax.rem(my_block + 1 + t, group // 2) * block_rows, block_rows)
        return pltpu.make_async_remote_copy(
            fbuf.at[j, pl.ds(row, block_rows)], rbuf.at[core * per_core + j],
            f_send.at[j, t], r_recv.at[core * per_core + j],
            device_id=(part, target), device_id_type=MESH,
        )

    @pl.when(jnp.logical_not(inner))
    def _():
        for i in range(2):
            outer_w(i).start()
        for j in range(per_core):
            for c in range(CORES):
                outer_e(j, c).start()

    @pl.when(inner)
    def _():
        for j in range(per_core):
            for c in range(CORES):
                far_e(j, c).start()
        near_w().start()
        for j in range(per_core):
            near_e(j).start()
        own_w().start()
        for j in range(per_core):
            own_e(j).start()

    for d in range(group - 1):
        mask_copy(d).start()
    mbuf[me] = mine_cols[...]

    @pl.when(inner)
    def _():
        def pass_on(j, carry):
            for c in range(CORES):
                arrived(ebuf.at[j, z_out * CORES + c], e_recv.at[j, z_out * CORES + c])
                onward_e(j, c).start()
            return carry

        for i in range(2):
            at, size = pieces[i]
            arrived(w_rows(out_block, my_quarter + at, size), w_recv.at[part, i])
            for d in range(PARTS - 1):
                plane_w(d, i).start()
        lax.fori_loop(0, per_core // 2, pass_on, 0)
        for i in range(2):
            at, size = pieces[i]
            for q in plane:
                arrived(w_rows(out_block, q * quarter + at, size), w_recv.at[q, i])
        across_w().start()
        own_w().wait()
        arrived(w_rows(in_other, 0, held), w_recv.at[PARTS, 0])
        lax.fori_loop(per_core // 2, per_core - 1, pass_on, 0)
        arrived(w_rows(out_other, 0, held), w_recv.at[PARTS, 1])

        mine_at = pl.multiple_of(half * half_rows, half_rows)
        theirs_at = pl.multiple_of((1 - half) * half_rows, half_rows)
        lanes = pl.ds(pl.multiple_of(half * span, 128), span)

        def finish(j):
            arrived(qbuf.at[j], p_recv.at[j])
            fbuf[j] = (keep[j] + qbuf[j].astype(jnp.float32)).astype(jnp.bfloat16)
            for t in range(group // 2 - 1):
                final_copy(j, t).start()
            own_row = pl.multiple_of(my_block * block_rows, block_rows)
            rbuf[core * per_core + j] = fbuf[j, pl.ds(own_row, block_rows)]

        def project(j, block, blocks):
            row = pl.multiple_of(block * block_rows, block_rows)

            def chunk(k, inside):
                start = pl.multiple_of(k * width, width)
                left = ebuf[j, pl.ds(block, blocks)].reshape(blocks * block_rows, features)
                zbuf[j, pl.ds(row, blocks * block_rows), pl.ds(start, width)] = lax.dot_general(
                    left, wbuf[pl.ds(start, width)], NT, preferred_element_type=jnp.float32
                ).astype(jnp.bfloat16)
                return inside

            lax.fori_loop(0, span // width, chunk, 0)

        def early(j, carry):
            @pl.when(j == per_core - 2)
            def _():
                pass_on(per_core - 1, 0)

            own_e(j).wait()
            arrived(ebuf.at[j, z_in * CORES + 1 - core], e_recv.at[j, z_in * CORES + 1 - core])
            for c in range(CORES):
                arrived(ebuf.at[j, z_far * CORES + c], e_recv.at[j, z_far * CORES + c])
            project(j, half * CORES, group - CORES)
            return carry

        lax.fori_loop(0, per_core, early, 0)

        def score(j, carry):
            for c in range(CORES):
                arrived(ebuf.at[j, far_out * CORES + c], e_recv.at[j, far_out * CORES + c])
            project(j, far_out * CORES, CORES)
            left = ebuf[j, :, :, lanes].reshape(rows, span)
            right = zbuf[j]
            sbuf[...] = lax.dot_general(
                left, right, NT, preferred_element_type=jnp.float32
            ) - lax.dot_general(right, left, NT, preferred_element_type=jnp.float32)
            pbuf[j] = sbuf[pl.ds(theirs_at, half_rows)].astype(jnp.bfloat16)
            partial_copy(j).start()
            keep[j] = sbuf[pl.ds(mine_at, half_rows)]

            @pl.when(j > 0)
            def _():
                finish(j - 1)

            return carry

        lax.fori_loop(0, per_core, score, 0)
        finish(per_core - 1)
        for j in range(per_core):
            arrived(rbuf.at[(1 - core) * per_core + j], r_recv.at[(1 - core) * per_core + j])
        for j in range(per_core):
            for c in range(CORES):
                far_e(j, c).wait_send()
                onward_e(j, c).wait_send()
            near_e(j).wait_send()
            partial_copy(j).wait_send()
            for t in range(group // 2 - 1):
                final_copy(j, t).wait_send()
        near_w().wait_send()
        across_w().wait_send()
        for d in range(PARTS - 1):
            for i in range(2):
                plane_w(d, i).wait_send()

    @pl.when(jnp.logical_not(inner))
    def _():
        for i in range(2):
            outer_w(i).wait_send()
        for j in range(per_core):
            for c in range(CORES):
                outer_e(j, c).wait_send()
        for p in range(prompts):
            arrived(rbuf.at[p], r_recv.at[p])

    for d in range(group - 1):
        mask_copy(d).wait_send()
        arrived(mbuf.at[others[d]], m_recv.at[others[d]])
    cols = mbuf[0]
    for g in range(1, group):
        cols = cols + mbuf[g]
    cols = cols.astype(jnp.float32)
    counts = jnp.sum(cols, axis=1, keepdims=True)
    pairs = jnp.maximum(counts - 1.0, 1.0)
    same = lax.broadcasted_iota(jnp.int32, (block_rows, block_rows), 0)
    same = (same == lax.broadcasted_iota(jnp.int32, (block_rows, block_rows), 1)).astype(jnp.float32)
    down = lax.dot_general(same, valid, NT, preferred_element_type=jnp.float32)
    lane = lax.broadcasted_iota(jnp.int32, (block_rows, 128), 1)
    rates = jnp.zeros((block_rows, 128), jnp.float32)
    for p in range(prompts):
        here = down[:, p:p + 1]
        prefs = jax.nn.sigmoid(rbuf[p].astype(jnp.float32)) * here * cols[p:p + 1, :]
        o_ref[p] = prefs
        totals = jnp.sum(prefs, axis=1, keepdims=True) - 0.5 * here
        rates = jnp.where(lane == p, here * totals / pairs[p:p + 1, :], rates)
    r_ref[...] = jnp.transpose(rates)[:prompts]


def line_scores(embeddings, head_weight, mask):
    prompts, block_rows, features = embeddings.shape
    held = head_weight.shape[0]
    group = CHIPS * CORES
    per_core = prompts // CORES
    span = held * group // 2
    rows = group * block_rows
    half_rows = rows // 2
    bf16, f32 = jnp.bfloat16, jnp.float32
    dma = pltpu.SemaphoreType.DMA
    anywhere = pl.BlockSpec(memory_space=pl.ANY)
    vmem = pl.BlockSpec(memory_space=pltpu.VMEM)
    return pl.pallas_call(
        kernel,
        out_shape=(
            jax.ShapeDtypeStruct((prompts, block_rows, rows), f32),
            jax.ShapeDtypeStruct((prompts, block_rows), f32),
        ),
        in_specs=[anywhere, anywhere, vmem],
        out_specs=(vmem, vmem),
        scratch_shapes=[
            pltpu.VMEM((per_core, group, block_rows, features), bf16),
            pltpu.VMEM((span, features), bf16),
            pltpu.VMEM((per_core, rows, span), bf16),
            pltpu.VMEM((rows, rows), f32),
            pltpu.VMEM((per_core, half_rows, rows), f32),
            pltpu.VMEM((per_core, half_rows, rows), bf16),
            pltpu.VMEM((per_core, half_rows, rows), bf16),
            pltpu.VMEM((per_core, half_rows, rows), bf16),
            pltpu.VMEM((prompts, block_rows, rows), bf16),
            pltpu.VMEM((prompts, rows), jnp.int32),
            pltpu.VMEM((group, prompts, rows), jnp.int32),
            dma((group - 1,)),
            dma((group,)),
            dma((per_core, 3)),
            dma((per_core, group)),
            dma((per_core, CORES)),
            dma((per_core,)),
            dma((PARTS + 1, 2)),
            dma((PARTS + 1, 2)),
            dma((1,)),
            dma((per_core,)),
            dma((per_core,)),
            dma((per_core, group // 2 - 1)),
            dma((prompts,)),
        ],
        compiler_params=pltpu.CompilerParams(
            collective_id=0, has_side_effects=True, vmem_limit_bytes=56 << 20
        ),
    )(embeddings, head_weight, mask)


def shards(embeddings, head_weight, valid_mask):
    group_size = lax.axis_size("resp")
    slots = group_size * embeddings.shape[1]
    if (lax.axis_size("prompt"), group_size) == (PARTS, CHIPS * CORES):
        return line_scores(embeddings, head_weight, valid_mask)
    valid_rows = valid_mask.astype(jnp.float32)
    counts = lax.psum(jnp.sum(valid_rows, axis=1), "resp")
    scores = gathered_scores(embeddings, head_weight)
    column_ids = jnp.arange(slots, dtype=jnp.float32)
    valid_cols = (column_ids[None, :] < counts[:, None]).astype(jnp.float32)
    preferences = jax.nn.sigmoid(scores) * valid_rows[:, :, None] * valid_cols[:, None, :]
    totals = jnp.sum(preferences, axis=2) - 0.5 * valid_rows
    win_rates = valid_rows * totals / jnp.maximum(counts - 1.0, 1.0)[:, None]
    return (preferences, win_rates)


def solution(mesh):
    return jax.shard_map(
        shards,
        mesh=mesh,
        in_specs=(P("prompt", "resp", None), P("resp", None), P("prompt", "resp")),
        out_specs=(P("prompt", "resp", None), P("prompt", "resp")),
        check_vma=False,
    )
```

```python
import functools

import jax
import jax.numpy as jnp
from jax import lax
from jax.experimental import pallas as pl
from jax.experimental.pallas import tpu as pltpu
from jax.sharding import PartitionSpec as P

MESH = pl.DeviceIdType.MESH
CORES = 2
CHIPS = 4
PARTS = 4
NT = (((1,), (1,)), ((), ()))


def gathered_halves(embeddings, head_weight, own_index, group_size):
    prompts, block_rows, features = embeddings.shape
    held = head_weight.shape[0]
    slots = group_size * block_rows
    everyone = lax.all_gather(embeddings, "resp", axis=0, tiled=True)
    flat = everyone.reshape(group_size * prompts * block_rows, features)
    through = lax.dot_general(flat, head_weight, NT, preferred_element_type=jnp.float32)
    through = through.astype(jnp.bfloat16).reshape(group_size, prompts, block_rows, held)
    mine = lax.dynamic_slice_in_dim(
        everyone.reshape(group_size, prompts, block_rows, features), own_index * held, held, 3
    )
    partial = jnp.einsum("gpid,hpjd->gpihj", mine, through, preferred_element_type=jnp.float32)
    flipped = jnp.einsum("gpid,hpjd->gpihj", through, mine, preferred_element_type=jnp.float32)
    partial = (partial - flipped).astype(jnp.bfloat16)
    return partial.reshape(group_size, prompts, block_rows, slots)


def gathered_scores(embeddings, head_weight):
    group_size = lax.axis_size("resp")
    own_index = lax.axis_index("resp")
    prompts, block_rows, features = embeddings.shape
    slots = group_size * block_rows
    at_once = max(1, min(prompts, (1 << 11) // slots))

    def scores_of(some):
        partial = gathered_halves(some, head_weight, own_index, group_size)
        swapped = lax.all_to_all(partial, "resp", split_axis=0, concat_axis=0, tiled=True)
        return jnp.sum(swapped.astype(jnp.float32), axis=0)

    pieces = embeddings.reshape(prompts // at_once, at_once, block_rows, features)
    return lax.map(scores_of, pieces).reshape(prompts, block_rows, slots)


def kernel(e_ref, w_ref, m_ref, o_ref, r_ref,
           ebuf, wbuf, zbuf, sbuf, keep, pbuf, qbuf, fbuf, rbuf, mine_cols, mbuf,
           m_send, m_recv, e_send, e_recv, ef_send, el_sem,
           w_send, w_recv, a_send, a_recv, wl_sem, p_send, p_recv, f_send, r_recv):
    part = lax.axis_index("prompt")
    me = lax.axis_index("resp")
    z = me // CORES
    core = me % CORES
    half = z // 2
    prompts, block_rows, features = e_ref.shape
    held = w_ref.shape[0]
    per_core = prompts // CORES
    group = CHIPS * CORES
    span = held * group // 2
    rows = group * block_rows
    half_rows = rows // 2
    z_in = 1 + half
    z_out = 3 * half
    z_far = 2 - half
    far_out = 3 - z_out
    inner = z == z_in
    quarter = held // PARTS
    width = 256 if span % 256 == 0 else span

    def copy(src, dst, send, recv, chip, c, q=None):
        return pltpu.make_async_remote_copy(
            src, dst, send, recv,
            device_id=(part if q is None else q, chip * CORES + c), device_id_type=MESH,
        )

    def arrived(dst, recv):
        copy(dst, dst, m_send.at[0], recv, z_far, core).wait_recv()

    valid = m_ref[...].astype(jnp.float32)
    slot = lax.broadcasted_iota(jnp.int32, (block_rows, rows), 1) - me * block_rows
    place = (slot == lax.broadcasted_iota(jnp.int32, (block_rows, rows), 0)).astype(jnp.float32)
    mine_cols[...] = jnp.dot(valid, place, preferred_element_type=jnp.float32).astype(jnp.int32)

    others = [lax.rem(me + d, group) for d in range(1, group)]
    plane = [lax.rem(part + d, PARTS) for d in range(1, PARTS)]
    barrier = pltpu.get_barrier_semaphore()
    for other in others:
        pl.semaphore_signal(barrier, inc=1, device_id=(part, other), device_id_type=MESH)
    for q in plane:
        pl.semaphore_signal(barrier, inc=1, device_id=(q, me), device_id_type=MESH)
    pl.semaphore_wait(barrier, len(others) + len(plane))

    def w_rows(block, start, size):
        return wbuf.at[pl.ds(pl.multiple_of(block * held + start, 16), size)]

    def mask_copy(d):
        return pltpu.make_async_remote_copy(
            mine_cols, mbuf.at[me], m_send.at[d], m_recv.at[me],
            device_id=(part, others[d]), device_id_type=MESH,
        )

    my_block = me - half * group // 2
    out_block = z_out * CORES + core - half * group // 2
    out_other = z_out * CORES + 1 - core - half * group // 2
    in_other = z_in * CORES + 1 - core - half * group // 2
    my_quarter = pl.multiple_of(part * quarter, 16)
    first = quarter // 32 * 16
    pieces = ((0, first), (first, quarter - first))

    def outer_w(i):
        at, size = pieces[i]
        return copy(w_ref.at[pl.ds(pl.multiple_of(my_quarter + at, 16), size)],
                    w_rows(my_block, my_quarter + at, size),
                    w_send.at[0, i], w_recv.at[part, i], z_in, core)

    def outer_e(j, c):
        return copy(e_ref.at[c * per_core + j], ebuf.at[j, me],
                    e_send.at[j, c], e_recv.at[j, me], z_in, c)

    def far_e(j, c):
        return copy(e_ref.at[c * per_core + j], ebuf.at[j, me],
                    e_send.at[j, c], e_recv.at[j, me], z_far, c)

    def near_e(j):
        return copy(e_ref.at[(1 - core) * per_core + j], ebuf.at[j, me],
                    e_send.at[j, 2], e_recv.at[j, me], z_in, 1 - core)

    def own_e(j):
        return pltpu.make_async_copy(e_ref.at[core * per_core + j], ebuf.at[j, me], el_sem.at[j])

    def onward_e(j, c):
        spot = ebuf.at[j, z_out * CORES + c]
        return copy(spot, spot, ef_send.at[j, c], e_recv.at[j, z_out * CORES + c], z_far, core)

    def near_w():
        return copy(w_ref, w_rows(my_block, 0, held), w_send.at[0, 0], w_recv.at[PARTS, 0], z_in, 1 - core)

    def own_w():
        return pltpu.make_async_copy(w_ref, w_rows(my_block, 0, held), wl_sem.at[0])

    def plane_w(d, i):
        at, size = pieces[i]
        spot = w_rows(out_block, my_quarter + at, size)
        return copy(spot, spot, w_send.at[1 + d, i], w_recv.at[part, i], z_in, core, plane[d])

    def across_w(q, i):
        at, size = pieces[i]
        spot = w_rows(out_block, q * quarter + at, size)
        return copy(spot, spot, a_send.at[q, i], a_recv.at[q, i], z_in, 1 - core)

    def partial_copy(j):
        return copy(pbuf.at[j], qbuf.at[j], p_send.at[j], p_recv.at[j], z_far, core)

    def final_copy(j, t):
        target = half * (group // 2) + lax.rem(my_block + 1 + t, group // 2)
        row = pl.multiple_of(lax.rem(my_block + 1 + t, group // 2) * block_rows, block_rows)
        return pltpu.make_async_remote_copy(
            fbuf.at[j, pl.ds(row, block_rows)], rbuf.at[core * per_core + j],
            f_send.at[j, t], r_recv.at[core * per_core + j],
            device_id=(part, target), device_id_type=MESH,
        )

    @pl.when(jnp.logical_not(inner))
    def _():
        for i in range(2):
            outer_w(i).start()
        for j in range(per_core):
            for c in range(CORES):
                outer_e(j, c).start()

    @pl.when(inner)
    def _():
        for j in range(per_core):
            for c in range(CORES):
                far_e(j, c).start()
        near_w().start()
        for j in range(per_core):
            near_e(j).start()
        own_w().start()
        for j in range(per_core):
            own_e(j).start()

    for d in range(group - 1):
        mask_copy(d).start()
    mbuf[me] = mine_cols[...]

    @pl.when(inner)
    def _():
        def pass_on(j, carry):
            for c in range(CORES):
                arrived(ebuf.at[j, z_out * CORES + c], e_recv.at[j, z_out * CORES + c])
                onward_e(j, c).start()
            return carry

        for i in range(2):
            at, size = pieces[i]
            arrived(w_rows(out_block, my_quarter + at, size), w_recv.at[part, i])
            for d in range(PARTS - 1):
                plane_w(d, i).start()
            across_w(part, i).start()
        lax.fori_loop(0, per_core // 2, pass_on, 0)
        for i in range(2):
            at, size = pieces[i]
            for q in plane:
                arrived(w_rows(out_block, q * quarter + at, size), w_recv.at[q, i])
                across_w(q, i).start()
        own_w().wait()
        arrived(w_rows(in_other, 0, held), w_recv.at[PARTS, 0])
        lax.fori_loop(per_core // 2, per_core - 1, pass_on, 0)
        for i in range(2):
            at, size = pieces[i]
            for q in range(PARTS):
                arrived(w_rows(out_other, q * quarter + at, size), a_recv.at[q, i])

        mine_at = pl.multiple_of(half * half_rows, half_rows)
        theirs_at = pl.multiple_of((1 - half) * half_rows, half_rows)
        lanes = pl.ds(pl.multiple_of(half * span, 128), span)

        def finish(j):
            arrived(qbuf.at[j], p_recv.at[j])
            fbuf[j] = (keep[j] + qbuf[j].astype(jnp.float32)).astype(jnp.bfloat16)
            for t in range(group // 2 - 1):
                final_copy(j, t).start()
            own_row = pl.multiple_of(my_block * block_rows, block_rows)
            rbuf[core * per_core + j] = fbuf[j, pl.ds(own_row, block_rows)]

        def project(j, many, block, blocks):
            row = pl.multiple_of(block * block_rows, block_rows)
            tall = blocks * block_rows

            def chunk(k, inside):
                start = pl.multiple_of(k * width, width)
                left = ebuf[pl.ds(j, many), pl.ds(block, blocks)].reshape(many * tall, features)
                zbuf[pl.ds(j, many), pl.ds(row, tall), pl.ds(start, width)] = lax.dot_general(
                    left, wbuf[pl.ds(start, width)], NT, preferred_element_type=jnp.float32
                ).astype(jnp.bfloat16).reshape(many, tall, width)
                return inside

            lax.fori_loop(0, span // width, chunk, 0)

        pair = per_core // 2

        def early(n, carry):
            @pl.when(n == 1)
            def _():
                pass_on(per_core - 1, 0)

            for i in range(pair):
                j = n * pair + i
                own_e(j).wait()
                arrived(ebuf.at[j, z_in * CORES + 1 - core], e_recv.at[j, z_in * CORES + 1 - core])
                for c in range(CORES):
                    arrived(ebuf.at[j, z_far * CORES + c], e_recv.at[j, z_far * CORES + c])
            project(n * pair, pair, half * CORES, group - CORES)
            return carry

        lax.fori_loop(0, 2, early, 0)

        def last_rows(j, carry):
            for c in range(CORES):
                arrived(ebuf.at[j, far_out * CORES + c], e_recv.at[j, far_out * CORES + c])
            return carry

        lax.fori_loop(0, per_core - 1, last_rows, 0)
        project(0, per_core - 1, far_out * CORES, CORES)

        def score(j, carry):
            @pl.when(j == per_core - 1)
            def _():
                last_rows(per_core - 1, 0)
                project(per_core - 1, 1, far_out * CORES, CORES)

            left = ebuf[j, :, :, lanes].reshape(rows, span)
            right = zbuf[j]
            sbuf[...] = lax.dot_general(
                left, right, NT, preferred_element_type=jnp.float32
            ) - lax.dot_general(right, left, NT, preferred_element_type=jnp.float32)
            pbuf[j] = sbuf[pl.ds(theirs_at, half_rows)].astype(jnp.bfloat16)
            partial_copy(j).start()
            keep[j] = sbuf[pl.ds(mine_at, half_rows)]

            @pl.when(j > 0)
            def _():
                finish(j - 1)

            return carry

        lax.fori_loop(0, per_core, score, 0)
        finish(per_core - 1)
        for j in range(per_core):
            arrived(rbuf.at[(1 - core) * per_core + j], r_recv.at[(1 - core) * per_core + j])
        for j in range(per_core):
            for c in range(CORES):
                far_e(j, c).wait_send()
                onward_e(j, c).wait_send()
            near_e(j).wait_send()
            partial_copy(j).wait_send()
            for t in range(group // 2 - 1):
                final_copy(j, t).wait_send()
        near_w().wait_send()
        for i in range(2):
            for q in range(PARTS):
                across_w(q, i).wait_send()
        for d in range(PARTS - 1):
            for i in range(2):
                plane_w(d, i).wait_send()

    @pl.when(jnp.logical_not(inner))
    def _():
        for i in range(2):
            outer_w(i).wait_send()
        for j in range(per_core):
            for c in range(CORES):
                outer_e(j, c).wait_send()
        for p in range(prompts):
            arrived(rbuf.at[p], r_recv.at[p])

    for d in range(group - 1):
        mask_copy(d).wait_send()
        arrived(mbuf.at[others[d]], m_recv.at[others[d]])
    cols = mbuf[0]
    for g in range(1, group):
        cols = cols + mbuf[g]
    cols = cols.astype(jnp.float32)
    counts = jnp.sum(cols, axis=1, keepdims=True)
    pairs = jnp.maximum(counts - 1.0, 1.0)
    same = lax.broadcasted_iota(jnp.int32, (block_rows, block_rows), 0)
    same = (same == lax.broadcasted_iota(jnp.int32, (block_rows, block_rows), 1)).astype(jnp.float32)
    down = lax.dot_general(same, valid, NT, preferred_element_type=jnp.float32)
    lane = lax.broadcasted_iota(jnp.int32, (block_rows, 128), 1)
    rates = jnp.zeros((block_rows, 128), jnp.float32)
    for p in range(prompts):
        here = down[:, p:p + 1]
        prefs = jax.nn.sigmoid(rbuf[p].astype(jnp.float32)) * here * cols[p:p + 1, :]
        o_ref[p] = prefs
        totals = jnp.sum(prefs, axis=1, keepdims=True) - 0.5 * here
        rates = jnp.where(lane == p, here * totals / pairs[p:p + 1, :], rates)
    r_ref[...] = jnp.transpose(rates)[:prompts]


def line_scores(embeddings, head_weight, mask):
    prompts, block_rows, features = embeddings.shape
    held = head_weight.shape[0]
    group = CHIPS * CORES
    per_core = prompts // CORES
    span = held * group // 2
    rows = group * block_rows
    half_rows = rows // 2
    bf16, f32 = jnp.bfloat16, jnp.float32
    dma = pltpu.SemaphoreType.DMA
    anywhere = pl.BlockSpec(memory_space=pl.ANY)
    vmem = pl.BlockSpec(memory_space=pltpu.VMEM)
    return pl.pallas_call(
        kernel,
        out_shape=(
            jax.ShapeDtypeStruct((prompts, block_rows, rows), f32),
            jax.ShapeDtypeStruct((prompts, block_rows), f32),
        ),
        in_specs=[anywhere, anywhere, vmem],
        out_specs=(vmem, vmem),
        scratch_shapes=[
            pltpu.VMEM((per_core, group, block_rows, features), bf16),
            pltpu.VMEM((span, features), bf16),
            pltpu.VMEM((per_core, rows, span), bf16),
            pltpu.VMEM((rows, rows), f32),
            pltpu.VMEM((per_core, half_rows, rows), f32),
            pltpu.VMEM((per_core, half_rows, rows), bf16),
            pltpu.VMEM((per_core, half_rows, rows), bf16),
            pltpu.VMEM((per_core, half_rows, rows), bf16),
            pltpu.VMEM((prompts, block_rows, rows), bf16),
            pltpu.VMEM((prompts, rows), jnp.int32),
            pltpu.VMEM((group, prompts, rows), jnp.int32),
            dma((group - 1,)),
            dma((group,)),
            dma((per_core, 3)),
            dma((per_core, group)),
            dma((per_core, CORES)),
            dma((per_core,)),
            dma((PARTS, 2)),
            dma((PARTS + 1, 1 + 1)),
            dma((PARTS, 2)),
            dma((PARTS, 2)),
            dma((1,)),
            dma((per_core,)),
            dma((per_core,)),
            dma((per_core, group // 2 - 1)),
            dma((prompts,)),
        ],
        compiler_params=pltpu.CompilerParams(
            collective_id=0, has_side_effects=True, vmem_limit_bytes=56 << 20
        ),
    )(embeddings, head_weight, mask)


def shards(embeddings, head_weight, valid_mask):
    group_size = lax.axis_size("resp")
    slots = group_size * embeddings.shape[1]
    if (lax.axis_size("prompt"), group_size) == (PARTS, CHIPS * CORES):
        return line_scores(embeddings, head_weight, valid_mask)
    valid_rows = valid_mask.astype(jnp.float32)
    counts = lax.psum(jnp.sum(valid_rows, axis=1), "resp")
    scores = gathered_scores(embeddings, head_weight)
    column_ids = jnp.arange(slots, dtype=jnp.float32)
    valid_cols = (column_ids[None, :] < counts[:, None]).astype(jnp.float32)
    preferences = jax.nn.sigmoid(scores) * valid_rows[:, :, None] * valid_cols[:, None, :]
    totals = jnp.sum(preferences, axis=2) - 0.5 * valid_rows
    win_rates = valid_rows * totals / jnp.maximum(counts - 1.0, 1.0)[:, None]
    return (preferences, win_rates)


def solution(mesh):
    return jax.shard_map(
        shards,
        mesh=mesh,
        in_specs=(P("prompt", "resp", None), P("resp", None), P("prompt", "resp")),
        out_specs=(P("prompt", "resp", None), P("prompt", "resp")),
        check_vma=False,
    )
```

```python
import functools

import jax
import jax.numpy as jnp
from jax import lax
from jax.experimental import pallas as pl
from jax.experimental.pallas import tpu as pltpu
from jax.sharding import PartitionSpec as P

MESH = pl.DeviceIdType.MESH
CORES = 2
CHIPS = 4
PARTS = 4
NT = (((1,), (1,)), ((), ()))


def gathered_halves(embeddings, head_weight, own_index, group_size):
    prompts, block_rows, features = embeddings.shape
    held = head_weight.shape[0]
    slots = group_size * block_rows
    everyone = lax.all_gather(embeddings, "resp", axis=0, tiled=True)
    flat = everyone.reshape(group_size * prompts * block_rows, features)
    through = lax.dot_general(flat, head_weight, NT, preferred_element_type=jnp.float32)
    through = through.astype(jnp.bfloat16).reshape(group_size, prompts, block_rows, held)
    mine = lax.dynamic_slice_in_dim(
        everyone.reshape(group_size, prompts, block_rows, features), own_index * held, held, 3
    )
    partial = jnp.einsum("gpid,hpjd->gpihj", mine, through, preferred_element_type=jnp.float32)
    flipped = jnp.einsum("gpid,hpjd->gpihj", through, mine, preferred_element_type=jnp.float32)
    partial = (partial - flipped).astype(jnp.bfloat16)
    return partial.reshape(group_size, prompts, block_rows, slots)


def gathered_scores(embeddings, head_weight):
    group_size = lax.axis_size("resp")
    own_index = lax.axis_index("resp")
    prompts, block_rows, features = embeddings.shape
    slots = group_size * block_rows
    at_once = max(1, min(prompts, (1 << 11) // slots))

    def scores_of(some):
        partial = gathered_halves(some, head_weight, own_index, group_size)
        swapped = lax.all_to_all(partial, "resp", split_axis=0, concat_axis=0, tiled=True)
        return jnp.sum(swapped.astype(jnp.float32), axis=0)

    pieces = embeddings.reshape(prompts // at_once, at_once, block_rows, features)
    return lax.map(scores_of, pieces).reshape(prompts, block_rows, slots)


def kernel(e_ref, w_ref, m_ref, o_ref, r_ref,
           ebuf, wbuf, zbuf, sbuf, keep, pbuf, qbuf, fbuf, rbuf, mine_cols, mbuf,
           m_send, m_recv, e_send, e_recv, ef_send, el_sem,
           w_send, w_recv, a_send, a_recv, wl_sem, p_send, p_recv, f_send, r_recv):
    part = lax.axis_index("prompt")
    me = lax.axis_index("resp")
    z = me // CORES
    core = me % CORES
    half = z // 2
    prompts, block_rows, features = e_ref.shape
    held = w_ref.shape[0]
    per_core = prompts // CORES
    group = CHIPS * CORES
    span = held * group // 2
    rows = group * block_rows
    half_rows = rows // 2
    z_in = 1 + half
    z_out = 3 * half
    z_far = 2 - half
    far_out = 3 - z_out
    inner = z == z_in
    quarter = held // PARTS
    width = 256 if span % 256 == 0 else span

    def copy(src, dst, send, recv, chip, c, q=None):
        return pltpu.make_async_remote_copy(
            src, dst, send, recv,
            device_id=(part if q is None else q, chip * CORES + c), device_id_type=MESH,
        )

    def arrived(dst, recv):
        copy(dst, dst, m_send.at[0], recv, z_far, core).wait_recv()

    valid = m_ref[...].astype(jnp.float32)
    slot = lax.broadcasted_iota(jnp.int32, (block_rows, rows), 1) - me * block_rows
    place = (slot == lax.broadcasted_iota(jnp.int32, (block_rows, rows), 0)).astype(jnp.float32)
    mine_cols[...] = jnp.dot(valid, place, preferred_element_type=jnp.float32).astype(jnp.int32)

    others = [lax.rem(me + d, group) for d in range(1, group)]
    plane = [lax.rem(part + d, PARTS) for d in range(1, PARTS)]
    barrier = pltpu.get_barrier_semaphore()
    for other in others:
        pl.semaphore_signal(barrier, inc=1, device_id=(part, other), device_id_type=MESH)
    for q in plane:
        pl.semaphore_signal(barrier, inc=1, device_id=(q, me), device_id_type=MESH)
    pl.semaphore_wait(barrier, len(others) + len(plane))

    def w_rows(block, start, size):
        return wbuf.at[pl.ds(pl.multiple_of(block * held + start, 16), size)]

    def mask_copy(d):
        return pltpu.make_async_remote_copy(
            mine_cols, mbuf.at[me], m_send.at[d], m_recv.at[me],
            device_id=(part, others[d]), device_id_type=MESH,
        )

    my_block = me - half * group // 2
    out_block = z_out * CORES + core - half * group // 2
    out_other = z_out * CORES + 1 - core - half * group // 2
    in_other = z_in * CORES + 1 - core - half * group // 2
    my_quarter = pl.multiple_of(part * quarter, 16)
    first = quarter // 32 * 16
    pieces = ((0, first), (first, quarter - first))

    def outer_w(i):
        at, size = pieces[i]
        return copy(w_ref.at[pl.ds(pl.multiple_of(my_quarter + at, 16), size)],
                    w_rows(my_block, my_quarter + at, size),
                    w_send.at[0, i], w_recv.at[part, i], z_in, core)

    def outer_e(j, c):
        return copy(e_ref.at[c * per_core + j], ebuf.at[j, me],
                    e_send.at[j, c], e_recv.at[j, me], z_in, c)

    def far_e(j, c):
        return copy(e_ref.at[c * per_core + j], ebuf.at[j, me],
                    e_send.at[j, c], e_recv.at[j, me], z_far, c)

    def near_e(j):
        return copy(e_ref.at[(1 - core) * per_core + j], ebuf.at[j, me],
                    e_send.at[j, 2], e_recv.at[j, me], z_in, 1 - core)

    def own_e(j):
        return pltpu.make_async_copy(e_ref.at[core * per_core + j], ebuf.at[j, me], el_sem.at[j])

    def onward_e(j, c):
        spot = ebuf.at[j, z_out * CORES + c]
        return copy(spot, spot, ef_send.at[j, c], e_recv.at[j, z_out * CORES + c], z_far, core)

    def near_w():
        return copy(w_ref, w_rows(my_block, 0, held), w_send.at[0, 0], w_recv.at[PARTS, 0], z_in, 1 - core)

    def own_w():
        return pltpu.make_async_copy(w_ref, w_rows(my_block, 0, held), wl_sem.at[0])

    def plane_w(d, i):
        at, size = pieces[i]
        spot = w_rows(out_block, my_quarter + at, size)
        return copy(spot, spot, w_send.at[1 + d, i], w_recv.at[part, i], z_in, core, plane[d])

    def across_w(q, i):
        at, size = pieces[i]
        spot = w_rows(out_block, q * quarter + at, size)
        return copy(spot, spot, a_send.at[q, i], a_recv.at[q, i], z_in, 1 - core)

    def partial_copy(j):
        return copy(pbuf.at[j], qbuf.at[j], p_send.at[j], p_recv.at[j], z_far, core)

    def final_copy(j, t):
        target = half * (group // 2) + lax.rem(my_block + 1 + t, group // 2)
        row = pl.multiple_of(lax.rem(my_block + 1 + t, group // 2) * block_rows, block_rows)
        return pltpu.make_async_remote_copy(
            fbuf.at[j, pl.ds(row, block_rows)], rbuf.at[core * per_core + j],
            f_send.at[j, t], r_recv.at[core * per_core + j],
            device_id=(part, target), device_id_type=MESH,
        )

    @pl.when(jnp.logical_not(inner))
    def _():
        for i in range(2):
            outer_w(i).start()
        for j in range(per_core):
            for c in range(CORES):
                outer_e(j, c).start()

    @pl.when(inner)
    def _():
        for j in range(per_core):
            for c in range(CORES):
                far_e(j, c).start()
        near_w().start()
        for j in range(per_core):
            near_e(j).start()
        own_w().start()
        for j in range(per_core):
            own_e(j).start()

    for d in range(group - 1):
        mask_copy(d).start()
    mbuf[me] = mine_cols[...]

    @pl.when(inner)
    def _():
        def pass_on(j, carry):
            for c in range(CORES):
                arrived(ebuf.at[j, z_out * CORES + c], e_recv.at[j, z_out * CORES + c])
                onward_e(j, c).start()
            return carry

        for i in range(2):
            at, size = pieces[i]
            arrived(w_rows(out_block, my_quarter + at, size), w_recv.at[part, i])
            for d in range(PARTS - 1):
                plane_w(d, i).start()
            across_w(part, i).start()
        lax.fori_loop(0, per_core // 2, pass_on, 0)
        for i in range(2):
            at, size = pieces[i]
            for q in plane:
                arrived(w_rows(out_block, q * quarter + at, size), w_recv.at[q, i])
                across_w(q, i).start()
        own_w().wait()
        arrived(w_rows(in_other, 0, held), w_recv.at[PARTS, 0])
        lax.fori_loop(per_core // 2, per_core - 1, pass_on, 0)
        for i in range(2):
            at, size = pieces[i]
            for q in range(PARTS):
                arrived(w_rows(out_other, q * quarter + at, size), a_recv.at[q, i])

        mine_at = pl.multiple_of(half * half_rows, half_rows)
        theirs_at = pl.multiple_of((1 - half) * half_rows, half_rows)
        lanes = pl.ds(pl.multiple_of(half * span, 128), span)

        def finish(j):
            arrived(qbuf.at[j], p_recv.at[j])
            fbuf[j] = (keep[j] + qbuf[j].astype(jnp.float32)).astype(jnp.bfloat16)
            for t in range(group // 2 - 1):
                final_copy(j, t).start()
            own_row = pl.multiple_of(my_block * block_rows, block_rows)
            rbuf[core * per_core + j] = fbuf[j, pl.ds(own_row, block_rows)]

        def project(j, many, block, blocks):
            row = pl.multiple_of(block * block_rows, block_rows)
            tall = blocks * block_rows

            def chunk(k, inside):
                start = pl.multiple_of(k * width, width)
                left = ebuf[pl.ds(j, many), pl.ds(block, blocks)].reshape(many * tall, features)
                zbuf[pl.ds(j, many), pl.ds(row, tall), pl.ds(start, width)] = lax.dot_general(
                    left, wbuf[pl.ds(start, width)], NT, preferred_element_type=jnp.float32
                ).astype(jnp.bfloat16).reshape(many, tall, width)
                return inside

            lax.fori_loop(0, span // width, chunk, 0)

        pair = per_core // 2

        def early(n, carry):
            @pl.when(n == 1)
            def _():
                pass_on(per_core - 1, 0)

            for i in range(pair):
                j = n * pair + i
                own_e(j).wait()
                arrived(ebuf.at[j, z_in * CORES + 1 - core], e_recv.at[j, z_in * CORES + 1 - core])
                for c in range(CORES):
                    arrived(ebuf.at[j, z_far * CORES + c], e_recv.at[j, z_far * CORES + c])
            project(n * pair, pair, half * CORES, group - CORES)
            return carry

        lax.fori_loop(0, 2, early, 0)

        def last_rows(j, carry):
            for c in range(CORES):
                arrived(ebuf.at[j, far_out * CORES + c], e_recv.at[j, far_out * CORES + c])
            return carry

        lax.fori_loop(0, per_core - 1, last_rows, 0)
        project(0, per_core - 1, far_out * CORES, CORES)

        def score(j, carry):
            @pl.when(j == per_core - 1)
            def _():
                last_rows(per_core - 1, 0)
                project(per_core - 1, 1, far_out * CORES, CORES)

            left = ebuf[j, :, :, lanes].reshape(rows, span)
            right = zbuf[j]
            sbuf[...] = lax.dot_general(
                left, right, NT, preferred_element_type=jnp.float32
            ) - lax.dot_general(right, left, NT, preferred_element_type=jnp.float32)
            pbuf[j] = sbuf[pl.ds(theirs_at, half_rows)].astype(jnp.bfloat16)
            partial_copy(j).start()
            keep[j] = sbuf[pl.ds(mine_at, half_rows)]
            return carry

        lax.fori_loop(0, per_core, score, 0)
        for j in range(per_core):
            finish(j)
        for j in range(per_core):
            arrived(rbuf.at[(1 - core) * per_core + j], r_recv.at[(1 - core) * per_core + j])
        for j in range(per_core):
            for c in range(CORES):
                far_e(j, c).wait_send()
                onward_e(j, c).wait_send()
            near_e(j).wait_send()
            partial_copy(j).wait_send()
            for t in range(group // 2 - 1):
                final_copy(j, t).wait_send()
        near_w().wait_send()
        for i in range(2):
            for q in range(PARTS):
                across_w(q, i).wait_send()
        for d in range(PARTS - 1):
            for i in range(2):
                plane_w(d, i).wait_send()

    @pl.when(jnp.logical_not(inner))
    def _():
        for i in range(2):
            outer_w(i).wait_send()
        for j in range(per_core):
            for c in range(CORES):
                outer_e(j, c).wait_send()
        for p in range(prompts):
            arrived(rbuf.at[p], r_recv.at[p])

    for d in range(group - 1):
        mask_copy(d).wait_send()
        arrived(mbuf.at[others[d]], m_recv.at[others[d]])
    cols = mbuf[0]
    for g in range(1, group):
        cols = cols + mbuf[g]
    cols = cols.astype(jnp.float32)
    counts = jnp.sum(cols, axis=1, keepdims=True)
    pairs = jnp.maximum(counts - 1.0, 1.0)
    same = lax.broadcasted_iota(jnp.int32, (block_rows, block_rows), 0)
    same = (same == lax.broadcasted_iota(jnp.int32, (block_rows, block_rows), 1)).astype(jnp.float32)
    down = lax.dot_general(same, valid, NT, preferred_element_type=jnp.float32)
    lane = lax.broadcasted_iota(jnp.int32, (block_rows, 128), 1)
    rates = jnp.zeros((block_rows, 128), jnp.float32)
    for p in range(prompts):
        here = down[:, p:p + 1]
        prefs = jax.nn.sigmoid(rbuf[p].astype(jnp.float32)) * here * cols[p:p + 1, :]
        o_ref[p] = prefs
        totals = jnp.sum(prefs, axis=1, keepdims=True) - 0.5 * here
        rates = jnp.where(lane == p, here * totals / pairs[p:p + 1, :], rates)
    r_ref[...] = jnp.transpose(rates)[:prompts]


def line_scores(embeddings, head_weight, mask):
    prompts, block_rows, features = embeddings.shape
    held = head_weight.shape[0]
    group = CHIPS * CORES
    per_core = prompts // CORES
    span = held * group // 2
    rows = group * block_rows
    half_rows = rows // 2
    bf16, f32 = jnp.bfloat16, jnp.float32
    dma = pltpu.SemaphoreType.DMA
    anywhere = pl.BlockSpec(memory_space=pl.ANY)
    vmem = pl.BlockSpec(memory_space=pltpu.VMEM)
    return pl.pallas_call(
        kernel,
        out_shape=(
            jax.ShapeDtypeStruct((prompts, block_rows, rows), f32),
            jax.ShapeDtypeStruct((prompts, block_rows), f32),
        ),
        in_specs=[anywhere, anywhere, vmem],
        out_specs=(vmem, vmem),
        scratch_shapes=[
            pltpu.VMEM((per_core, group, block_rows, features), bf16),
            pltpu.VMEM((span, features), bf16),
            pltpu.VMEM((per_core, rows, span), bf16),
            pltpu.VMEM((rows, rows), f32),
            pltpu.VMEM((per_core, half_rows, rows), f32),
            pltpu.VMEM((per_core, half_rows, rows), bf16),
            pltpu.VMEM((per_core, half_rows, rows), bf16),
            pltpu.VMEM((per_core, half_rows, rows), bf16),
            pltpu.VMEM((prompts, block_rows, rows), bf16),
            pltpu.VMEM((prompts, rows), jnp.int32),
            pltpu.VMEM((group, prompts, rows), jnp.int32),
            dma((group - 1,)),
            dma((group,)),
            dma((per_core, 3)),
            dma((per_core, group)),
            dma((per_core, CORES)),
            dma((per_core,)),
            dma((PARTS, 2)),
            dma((PARTS + 1, 1 + 1)),
            dma((PARTS, 2)),
            dma((PARTS, 2)),
            dma((1,)),
            dma((per_core,)),
            dma((per_core,)),
            dma((per_core, group // 2 - 1)),
            dma((prompts,)),
        ],
        compiler_params=pltpu.CompilerParams(
            collective_id=0, has_side_effects=True, vmem_limit_bytes=56 << 20
        ),
    )(embeddings, head_weight, mask)


def shards(embeddings, head_weight, valid_mask):
    group_size = lax.axis_size("resp")
    slots = group_size * embeddings.shape[1]
    if (lax.axis_size("prompt"), group_size) == (PARTS, CHIPS * CORES):
        return line_scores(embeddings, head_weight, valid_mask)
    valid_rows = valid_mask.astype(jnp.float32)
    counts = lax.psum(jnp.sum(valid_rows, axis=1), "resp")
    scores = gathered_scores(embeddings, head_weight)
    column_ids = jnp.arange(slots, dtype=jnp.float32)
    valid_cols = (column_ids[None, :] < counts[:, None]).astype(jnp.float32)
    preferences = jax.nn.sigmoid(scores) * valid_rows[:, :, None] * valid_cols[:, None, :]
    totals = jnp.sum(preferences, axis=2) - 0.5 * valid_rows
    win_rates = valid_rows * totals / jnp.maximum(counts - 1.0, 1.0)[:, None]
    return (preferences, win_rates)


def solution(mesh):
    return jax.shard_map(
        shards,
        mesh=mesh,
        in_specs=(P("prompt", "resp", None), P("resp", None), P("prompt", "resp")),
        out_specs=(P("prompt", "resp", None), P("prompt", "resp")),
        check_vma=False,
    )
```
